32 devices in a mesh: batch: 2 (over x), row: 4 (over z), col: 4 (over y, core).
Axes of the slice: x: 2, y: 2, z: 4, core: 2. Of those that a mesh axis runs over, the one named last changes fastest.
Arguments:
- tri_mat: bfloat16 [28672, 14336], P(('batch', 'row'), 'col'), parts along dimension 0
- rhs_mat: bfloat16 [28672, 4096], P(('batch', 'row'), 'col'), parts along dimension 0
Outputs:
- output: bfloat16 [28672, 4096], P(('batch', 'row'), 'col'), parts along dimension 0
There are 2 independent parts. The reference program is written for one: setup_inputs(seed, part) draws one part's arguments, and reference() takes and returns one part's arrays. A program takes and returns all parts, laid end to end along the dimension named above; each array names one.
All inputs are finite; a program needn't handle non-finite values.
Results may differ from the reference program's by a relative error of at most 0.001.
Values are sent between devices in bfloat16 or wider.
A program may use at most 1 GiB of HBM per device.

```python
import jax
import jax.numpy as jnp

MAT_ORDER = 14336
BLOCK_SIZE = 256
COLS_DEV = 1024
GRID_ROWS = 4
GRID_COLS = 4
NUM_COLS = COLS_DEV * GRID_COLS
NUM_BLOCKS = MAT_ORDER // BLOCK_SIZE


def logical_index(grid_size):
    stored = jnp.arange(MAT_ORDER, dtype=jnp.int32)
    block_idx = stored // BLOCK_SIZE
    per_device = NUM_BLOCKS // grid_size
    owner_dev = block_idx // per_device
    local_blk = block_idx % per_device
    return (local_blk * grid_size + owner_dev) * BLOCK_SIZE + stored % BLOCK_SIZE


def setup_inputs(seed: int = 0, part: int = 0) -> dict:
    base_key = jax.random.fold_in(jax.random.key(seed), part)
    key_tri, key_rhs = jax.random.split(base_key)
    row_ids = logical_index(GRID_ROWS)
    col_ids = logical_index(GRID_COLS)
    lower_mask = row_ids[:, None] >= col_ids[None, :]
    scale_tri = MAT_ORDER ** -0.5
    draws = jax.random.normal(key_tri, (MAT_ORDER, MAT_ORDER), jnp.float32) * scale_tri
    tri_mat = jnp.where(lower_mask, draws, 0.0).astype(jnp.bfloat16)
    rhs_mat = jax.random.normal(key_rhs, (MAT_ORDER, NUM_COLS), jnp.float32).astype(jnp.bfloat16)
    return {"tri_mat": tri_mat, "rhs_mat": rhs_mat}


def reference(tri_mat, rhs_mat):
    by_rows = rhs_mat.reshape(GRID_ROWS, NUM_BLOCKS // GRID_ROWS, BLOCK_SIZE, NUM_COLS)
    logical = by_rows.transpose(1, 0, 2, 3).reshape(NUM_BLOCKS // GRID_COLS, GRID_COLS, BLOCK_SIZE, NUM_COLS)
    rhs_by_cols = logical.transpose(1, 0, 2, 3).reshape(MAT_ORDER, NUM_COLS)
    product = jnp.dot(tri_mat, rhs_by_cols, preferred_element_type=jnp.float32)
    return product.astype(jnp.bfloat16)
```

```python
import functools

import jax
import jax.numpy as jnp
from jax import lax
from jax.experimental import pallas as pl
from jax.experimental.pallas import tpu as pltpu
from jax.sharding import PartitionSpec as P

BLOCK_SIZE = 256
NEAR_STEPS = 6
LAG = 3
AHEAD = 4
SLOTS = 4
MESH = pl.DeviceIdType.MESH


def flip(v, t):
    if t == 0:
        return v
    if t == 1:
        return v + 1 - 2 * lax.rem(v, 2)
    if t == 2:
        return lax.rem(v + 2, 4)
    return 3 - v


def xor(a, b):
    return lax.rem(a + b, 2) + 2 * lax.rem(a // 2 + b // 2, 2)


def kernel(bs, nb, near, tri, rhs, out, l_got, l_end, b_got, acc, part, l_tile, b_tile, o_tile, sems, l_sem, b_sem, o_sem):
    (ys, yr, ds, dr, fs, fr, b1s, b1r, l0s, l0r, l2s, l2r, e0s, e0r, e2s, e2r,
     os_, or_, ws, wr, ms, mr, us, ur, vs, vr, ps, pr) = sems
    g, z, c = lax.axis_index("batch"), lax.axis_index("row"), lax.axis_index("col")
    is_end = lax.rem(z, 3) == 0
    ze = flip(z, 1)
    zo = flip(z, 3)
    sib, across = flip(c, 1), flip(c, 2)

    def rows(s):
        return pl.ds(pl.multiple_of(s * bs, bs), bs)

    def panel(ref, s, n=None):
        at = (pl.ds(s * bs, (nb - s) * bs), pl.ds(s * bs, bs))
        return ref.at[at] if n is None else ref.at[(n,) + at]

    def send(src, dst, ss, rs, dev):
        return pltpu.make_async_remote_copy(src_ref=src, dst_ref=dst, send_sem=ss, recv_sem=rs, device_id=dev, device_id_type=MESH)

    def y_copy(s):
        return send(panel(tri, s), panel(l_got, s, 1), ys.at[s], yr.at[s], (g, z, across))

    def d_copy(s):
        return send(panel(tri, s), panel(l_got, s, 0), ds.at[s], dr.at[s], (g, z, sib))

    def f_copy(s):
        return send(panel(l_got, s, 1), panel(l_got, s, 2), fs.at[s], fr.at[s], (g, z, sib))

    def l0_copy(s):
        return send(panel(tri, s), panel(l_end, s, 0), l0s.at[s - near], l0r.at[s - near], (g, ze, c))

    def l2_copy(s):
        return send(panel(l_got, s, 1), panel(l_end, s, 2), l2s.at[s - near], l2r.at[s - near], (g, ze, c))

    def e0_copy(s):
        return send(panel(l_end, s, 0), panel(l_end, s, 1), e0s.at[s - near], e0r.at[s - near], (g, z, sib))

    def e2_copy(s):
        return send(panel(l_end, s, 2), panel(l_end, s, 3), e2s.at[s - near], e2r.at[s - near], (g, z, sib))

    def b_copy(owner, n, ss, rs, dev):
        return send(rhs.at[rows(n)], b_got.at[owner, rows(n)], ss.at[n], rs.at[n], dev)

    def b_forward(owner, n, ss, rs, dev):
        return send(b_got.at[owner, rows(n)], b_got.at[owner, rows(n)], ss.at[n], rs.at[n], dev)

    def b1_copy(n):
        return b_copy(z, n, b1s, b1r, (g, ze, c))

    def o_copy(n):
        return b_copy(z, n, os_, or_, (g, zo, c))

    def w_copy(n):
        return b_forward(ze, n, ws, wr, (g, zo, c))

    def m_copy(n):
        return b_copy(z, n, ms, mr, (g, ze, c))

    def u_copy(n):
        return b_forward(zo, n, us, ur, (g, ze, c))

    def v_copy(n):
        return b_forward(flip(zo, 1), n, vs, vr, (g, ze, c))

    def p_copy(j):
        at = pl.ds(pl.multiple_of((j - near) * bs, bs), bs)
        return send(part.at[at], part.at[at], ps.at[j - near], pr.at[j - near], (g, ze, c))

    def at_step(s, lo, hi, fn):
        for i in range(lo, hi):
            @pl.when(s == i)
            def _():
                fn(i)

    def pass_on(s):
        y_copy(s).wait_recv()
        f_copy(s).start()

    def load_b(slots):
        for i, owner in slots:
            to = b_tile.at[pl.ds(i * bs, bs)]

            @pl.when(owner == z)
            def _():
                pltpu.make_async_copy(rhs.at[rows(load_b.step)], to, b_sem.at[i]).start()

            @pl.when(owner != z)
            def _():
                pltpu.make_async_copy(b_got.at[owner, rows(load_b.step)], to, b_sem.at[i]).start()
        for i, owner in slots:
            pltpu.make_async_copy(rhs.at[rows(0)], b_tile.at[pl.ds(i * bs, bs)], b_sem.at[i]).wait()

    def tiles(s, start_tile, depth, target, base):
        def start(j):
            start_tile(j, lax.rem(j - s, SLOTS))

        def wait(slot):
            for i in range(depth):
                to = l_tile.at[slot, :, pl.ds(i * bs, bs)]
                pltpu.make_async_copy(tri.at[pl.ds(0, bs), pl.ds(0, bs)], to, l_sem.at[slot, i]).wait()

        for d in range(SLOTS - 1):
            @pl.when(s + d < nb)
            def _():
                start(s + d)

        @pl.loop(s, nb)
        def _(j):
            @pl.when(j + SLOTS - 1 < nb)
            def _():
                start(j + SLOTS - 1)

            slot = lax.rem(j - s, SLOTS)
            wait(slot)
            at = pl.ds(pl.multiple_of((j - base) * bs, bs), bs)
            target[at, :] += jnp.dot(
                l_tile[slot, :, : depth * bs], b_tile[: depth * bs, :], preferred_element_type=jnp.float32
            )

    def l_copy(ref, j, s, slot, i):
        to = l_tile.at[slot, :, pl.ds(i * bs, bs)]
        return pltpu.make_async_copy(ref.at[rows(j), rows(s)], to, l_sem.at[slot, i])

    def own_step(s):
        load_b.step = s
        load_b([(r, flip(c, r)) for r in range(4)])

        def start_tile(j, slot):
            l_copy(tri, j, s, slot, 0).start()
            for r in range(1, 4):
                l_copy(l_got.at[r - 1], j, s, slot, r).start()

        tiles(s, start_tile, 4, acc, 0)

    def diag_step(s):
        load_b.step = s
        load_b([(0, z)])
        r = xor(c, z)

        def start_tile(j, slot):
            @pl.when(r == 0)
            def _():
                l_copy(tri, j, s, slot, 0).start()

            for k in range(1, 4):
                @pl.when(r == k)
                def _():
                    l_copy(l_got.at[k - 1], j, s, slot, 0).start()

        tiles(s, start_tile, 1, acc, 0)

    def end_step(s):
        load_b.step = s
        load_b([(t - 1, flip(ze, t)) for t in range(1, 4)])
        r0 = xor(c, ze)

        def start_tile(j, slot):
            for t in range(1, 4):
                l_copy(l_end.at[flip(r0, t)], j, s, slot, t - 1).start()

        tiles(s, start_tile, 3, part, near)

    def finish(j, extra):
        at = rows(j)
        total = acc[at, :]
        if extra:
            total = total + part[pl.ds(pl.multiple_of((j - near) * bs, bs), bs), :]
        o_tile[...] = total.astype(o_tile.dtype)
        copy = pltpu.make_async_copy(o_tile, out.at[at], o_sem)
        copy.start()
        copy.wait()

    has0, has2 = c != ze, across != ze
    gives0, gives2 = c != z, across != z

    @pl.when(is_end)
    def _():
        for s in list(range(near, nb)) + list(range(near)):
            y_copy(s).start()
        for s in range(nb):
            d_copy(s).start()
        sent = 0
        for j in range(near, nb):
            upto = min(4 + 2 * (j - near), j + 2) if j < nb - 1 else nb - 2
            for n in range(sent, upto):
                b1_copy(n).start()
            sent = max(sent, upto)
            pass_on(j)

            @pl.when(gives0)
            def _():
                l0_copy(j).start()

            @pl.when(gives2)
            def _():
                l2_copy(j).start()

        for n in range(sent, nb):
            b1_copy(n).start()

        acc[...] = jnp.zeros_like(acc)

        @pl.loop(near, nb)
        def _(s):
            def ready(i):
                d_copy(i).wait_recv()
                f_copy(i).wait_recv()

            at_step(s, near, nb, ready)
            diag_step(s)

        @pl.loop(0, near)
        def _(s):
            def ready(i):
                pass_on(i)
                d_copy(i).wait_recv()
                f_copy(i).wait_recv()

            at_step(s, 0, near, ready)
            for copy in (m_copy, u_copy, v_copy):
                copy(s).wait_recv()
            own_step(s)
            finish(s, False)

        @pl.loop(near, nb)
        def _(j):
            p_copy(j).wait_recv()
            finish(j, True)

        for s in range(nb):
            y_copy(s).wait_send()
            d_copy(s).wait_send()
            f_copy(s).wait_send()
            b1_copy(s).wait_send()
        for s in range(near, nb):
            @pl.when(gives0)
            def _():
                l0_copy(s).wait_send()

            @pl.when(gives2)
            def _():
                l2_copy(s).wait_send()

    @pl.when(jnp.logical_not(is_end))
    def _():
        for n in range(AHEAD):
            o_copy(n).start()
        for n in range(near):
            m_copy(n).start()
        for s in range(nb):
            y_copy(s).start()
        for s in range(nb):
            d_copy(s).start()
        acc[...] = jnp.zeros_like(acc)
        part[...] = jnp.zeros_like(part)

        @pl.loop(0, nb + LAG)
        def _(n):
            @pl.when(n < nb)
            def _():
                b1_copy(n).wait_recv()
                w_copy(n).start()

                @pl.when(n + AHEAD < nb)
                def _():
                    o_copy(n + AHEAD).start()

                o_copy(n).wait_recv()
                w_copy(n).wait_recv()

                @pl.when(n < near)
                def _():
                    u_copy(n).start()
                    v_copy(n).start()

                @pl.when(n >= near)
                def _():
                    def relay(i):
                        @pl.when(has0)
                        def _():
                            l0_copy(i).wait_recv()
                            e0_copy(i).start()

                        @pl.when(has2)
                        def _():
                            l2_copy(i).wait_recv()
                            e2_copy(i).start()

                        @pl.when(sib != ze)
                        def _():
                            e0_copy(i).wait_recv()

                        @pl.when(3 - c != ze)
                        def _():
                            e2_copy(i).wait_recv()

                    at_step(n, near, nb, relay)
                    end_step(n)
                    p_copy(n).start()

            @pl.when(n >= LAG)
            def _():
                s = n - LAG

                def ready(i):
                    pass_on(i)
                    d_copy(i).wait_recv()
                    f_copy(i).wait_recv()

                at_step(s, 0, nb, ready)
                own_step(s)
                finish(s, False)

        for s in range(nb):
            y_copy(s).wait_send()
            d_copy(s).wait_send()
            f_copy(s).wait_send()
            o_copy(s).wait_send()
            w_copy(s).wait_send()
        for s in range(near):
            m_copy(s).wait_send()
            u_copy(s).wait_send()
            v_copy(s).wait_send()
        for s in range(near, nb):
            p_copy(s).wait_send()

            @pl.when(has0)
            def _():
                e0_copy(s).wait_send()

            @pl.when(has2)
            def _():
                e2_copy(s).wait_send()


def local_trmm(tri, rhs, bs=BLOCK_SIZE, near=NEAR_STEPS):
    size, cols = rhs.shape
    nb = size // bs
    far = nb - near
    any_spec = pl.BlockSpec(memory_space=pl.ANY)
    counts = [nb] * 8 + [far] * 8 + [nb] * 4 + [near] * 6 + [far] * 2
    return pl.pallas_call(
        functools.partial(kernel, bs, nb, near),
        out_shape=[
            jax.ShapeDtypeStruct((size, cols), jnp.bfloat16),
            jax.ShapeDtypeStruct((3, size, size), jnp.bfloat16),
            jax.ShapeDtypeStruct((4, size, size), jnp.bfloat16),
            jax.ShapeDtypeStruct((4, size, cols), jnp.bfloat16),
        ],
        in_specs=[any_spec] * 2,
        out_specs=[any_spec] * 4,
        scratch_shapes=[
            pltpu.VMEM((size, cols), jnp.float32),
            pltpu.VMEM((far * bs, cols), jnp.float32),
            pltpu.VMEM((SLOTS, bs, 4 * bs), jnp.bfloat16),
            pltpu.VMEM((4 * bs, cols), jnp.bfloat16),
            pltpu.VMEM((bs, cols), jnp.bfloat16),
            tuple(pltpu.SemaphoreType.DMA((n,)) for n in counts),
            pltpu.SemaphoreType.DMA((SLOTS, 4)),
            pltpu.SemaphoreType.DMA((4,)),
            pltpu.SemaphoreType.DMA,
        ],
        compiler_params=pltpu.CompilerParams(has_side_effects=True, vmem_limit_bytes=56 * 2**20),
    )(tri, rhs)[0]


def solution(mesh):
    part_spec = P(("batch", "row"), "col")
    return jax.shard_map(local_trmm, mesh=mesh, in_specs=(part_spec, part_spec), out_specs=part_spec, check_vma=False)
```

```python
import functools

import jax
import jax.numpy as jnp
from jax import lax
from jax.experimental import pallas as pl
from jax.experimental.pallas import tpu as pltpu
from jax.sharding import PartitionSpec as P

BLOCK_SIZE = 256
NEAR_STEPS = 6
AHEAD = 1
SLOTS = 5
MESH = pl.DeviceIdType.MESH


def flip(v, t):
    if t == 0:
        return v
    if t == 1:
        return v + 1 - 2 * lax.rem(v, 2)
    if t == 2:
        return lax.rem(v + 2, 4)
    return 3 - v


def xor(a, b):
    return lax.rem(a + b, 2) + 2 * lax.rem(a // 2 + b // 2, 2)


def kernel(bs, nb, near, tri, rhs, out, l_got, l_end, b_got, acc, part, l_tile, b_tile, o_tile, sems, l_sem, b_sem, o_sem):
    (ys, yr, ds, dr, fs, fr, b1s, b1r, l0s, l0r, l2s, l2r, e0s, e0r, e2s, e2r, l3s, l3r, e3s, e3r,
     os_, or_, ws, wr, ms, mr, us, ur, vs, vr, ps, pr) = sems
    g, z, c = lax.axis_index("batch"), lax.axis_index("row"), lax.axis_index("col")
    is_end = lax.rem(z, 3) == 0
    ze = flip(z, 1)
    zo = flip(z, 3)
    sib, across = flip(c, 1), flip(c, 2)

    def rows(s):
        return pl.ds(pl.multiple_of(s * bs, bs), bs)

    def panel(ref, s, n=None):
        at = (pl.ds(s * bs, (nb - s) * bs), pl.ds(s * bs, bs))
        return ref.at[at] if n is None else ref.at[(n,) + at]

    def send(src, dst, ss, rs, dev):
        return pltpu.make_async_remote_copy(src_ref=src, dst_ref=dst, send_sem=ss, recv_sem=rs, device_id=dev, device_id_type=MESH)

    def y_copy(s):
        return send(panel(tri, s), panel(l_got, s, 1), ys.at[s], yr.at[s], (g, z, across))

    def d_copy(s):
        return send(panel(tri, s), panel(l_got, s, 0), ds.at[s], dr.at[s], (g, z, sib))

    def f_copy(s):
        return send(panel(l_got, s, 1), panel(l_got, s, 2), fs.at[s], fr.at[s], (g, z, sib))

    def l0_copy(s):
        return send(panel(tri, s), panel(l_end, s, 0), l0s.at[s - near], l0r.at[s - near], (g, ze, c))

    def l2_copy(s):
        return send(panel(l_got, s, 1), panel(l_end, s, 2), l2s.at[s - near], l2r.at[s - near], (g, ze, c))

    def e0_copy(s):
        return send(panel(l_end, s, 0), panel(l_end, s, 1), e0s.at[s - near], e0r.at[s - near], (g, z, sib))

    def e2_copy(s):
        return send(panel(l_end, s, 2), panel(l_end, s, 3), e2s.at[s - near], e2r.at[s - near], (g, z, sib))

    def l3_copy(s):
        return send(panel(l_got, s, 2), panel(l_end, s, 3), l3s.at[s - near], l3r.at[s - near], (g, ze, c))

    def e3_copy(s):
        return send(panel(l_end, s, 3), panel(l_end, s, 2), e3s.at[s - near], e3r.at[s - near], (g, z, sib))

    def b_copy(owner, n, ss, rs, dev):
        return send(rhs.at[rows(n)], b_got.at[owner, rows(n)], ss.at[n], rs.at[n], dev)

    def b_forward(owner, n, ss, rs, dev):
        return send(b_got.at[owner, rows(n)], b_got.at[owner, rows(n)], ss.at[n], rs.at[n], dev)

    def b1_copy(n):
        return b_copy(z, n, b1s, b1r, (g, ze, c))

    def o_copy(n):
        return b_copy(z, n, os_, or_, (g, zo, c))

    def w_copy(n):
        return b_forward(ze, n, ws, wr, (g, zo, c))

    def m_copy(n):
        return b_copy(z, n, ms, mr, (g, ze, c))

    def u_copy(n):
        return b_forward(zo, n, us, ur, (g, ze, c))

    def v_copy(n):
        return b_forward(flip(zo, 1), n, vs, vr, (g, ze, c))

    def p_copy(j):
        at = pl.ds(pl.multiple_of((j - near) * bs, bs), bs)
        return send(part.at[at], part.at[at], ps.at[j - near], pr.at[j - near], (g, ze, c))

    def at_step(s, lo, hi, fn):
        for i in range(lo, hi):
            @pl.when(s == i)
            def _():
                fn(i)

    def pass_on(s):
        y_copy(s).wait_recv()
        f_copy(s).start()

    def load_b(slots):
        for i, owner in slots:
            to = b_tile.at[pl.ds(i * bs, bs)]

            @pl.when(owner == z)
            def _():
                pltpu.make_async_copy(rhs.at[rows(load_b.step)], to, b_sem.at[i]).start()

            @pl.when(owner != z)
            def _():
                pltpu.make_async_copy(b_got.at[owner, rows(load_b.step)], to, b_sem.at[i]).start()

    def tiles(s, start_tile, depth, target, base, after_first=None):
        def start(j):
            start_tile(j, lax.rem(j - s, SLOTS))

        def wait(slot):
            for i in range(depth):
                to = l_tile.at[slot, :, pl.ds(i * bs, bs)]
                pltpu.make_async_copy(tri.at[pl.ds(0, bs), pl.ds(0, bs)], to, l_sem.at[slot, i]).wait()

        for d in range(SLOTS - 1):
            @pl.when(s + d < nb)
            def _():
                start(s + d)
        for i in range(depth):
            pltpu.make_async_copy(rhs.at[rows(0)], b_tile.at[pl.ds(i * bs, bs)], b_sem.at[i]).wait()

        @pl.loop(s, nb)
        def _(j):
            @pl.when(j + SLOTS - 1 < nb)
            def _():
                start(j + SLOTS - 1)

            slot = lax.rem(j - s, SLOTS)
            wait(slot)
            if after_first is not None:
                @pl.when(j == s + 1)
                def _():
                    after_first()

            at = pl.ds(pl.multiple_of((j - base) * bs, bs), bs)
            target[at, :] += jnp.dot(
                l_tile[slot, :, : depth * bs], b_tile[: depth * bs, :], preferred_element_type=jnp.float32
            )

    def l_copy(ref, j, s, slot, i):
        to = l_tile.at[slot, :, pl.ds(i * bs, bs)]
        return pltpu.make_async_copy(ref.at[rows(j), rows(s)], to, l_sem.at[slot, i])

    def own_step(s):
        load_b.step = s
        load_b([(r, flip(c, r)) for r in range(4)])

        def start_tile(j, slot):
            l_copy(tri, j, s, slot, 0).start()
            for r in range(1, 4):
                l_copy(l_got.at[r - 1], j, s, slot, r).start()

        tiles(s, start_tile, 4, acc, 0)

    def diag_step(s):
        load_b.step = s
        load_b([(0, z)])
        r = xor(c, z)

        def start_tile(j, slot):
            @pl.when(r == 0)
            def _():
                l_copy(tri, j, s, slot, 0).start()

            for k in range(1, 4):
                @pl.when(r == k)
                def _():
                    l_copy(l_got.at[k - 1], j, s, slot, 0).start()

        tiles(s, start_tile, 1, acc, 0)

    def end_step(s):
        load_b.step = s
        load_b([(t - 1, flip(ze, t)) for t in range(1, 4)])
        r0 = xor(c, ze)

        def start_tile(j, slot):
            for t in range(1, 4):
                l_copy(l_end.at[flip(r0, t)], j, s, slot, t - 1).start()

        tiles(s, start_tile, 3, part, near, lambda: p_copy(s).start())

        @pl.when(s == nb - 1)
        def _():
            p_copy(s).start()

    def finish(j, extra):
        at = rows(j)
        total = acc[at, :]
        if extra:
            total = total + part[pl.ds(pl.multiple_of((j - near) * bs, bs), bs), :]
        slot = lax.rem(j, 2)

        @pl.when(j >= 2)
        def _():
            o_copy_out(j - 2).wait()

        o_tile[slot] = total.astype(o_tile.dtype)
        o_copy_out(j).start()

    def o_copy_out(j):
        slot = lax.rem(j, 2)
        return pltpu.make_async_copy(o_tile.at[slot], out.at[rows(j)], o_sem.at[slot])

    gives0, gives2 = c != z, across != z
    has0, has2 = c != ze, across != ze
    light = lax.rem(c + z, 2) == 0
    light_there = lax.rem(c + ze, 2) == 0
    heavy, heavy_there = jnp.logical_not(light), jnp.logical_not(light_there)

    def swapped(s):
        return (s - near) % 2 == 1

    def over2(s):
        return jnp.logical_and(gives2, light) if swapped(s) else gives2

    def got2(s):
        return jnp.logical_and(has2, light_there) if swapped(s) else has2

    @pl.when(is_end)
    def _():
        for s in list(range(near, nb)) + list(range(near)):
            y_copy(s).start()
        for s in range(nb):
            d_copy(s).start()
        order = sorted([(2 * n + 1, n, False) for n in range(nb)] + [(2 * j + 2, j, True) for j in range(near, nb)])
        for _, i, is_l in order:
            if not is_l:
                b1_copy(i).start()
                continue
            pass_on(i)

            @pl.when(gives0)
            def _():
                l0_copy(i).start()

            @pl.when(over2(i))
            def _():
                l2_copy(i).start()

            if swapped(i):
                @pl.when(light)
                def _():
                    f_copy(i).wait_recv()
                    l3_copy(i).start()

        acc[...] = jnp.zeros_like(acc)

        @pl.loop(near, nb)
        def _(s):
            def ready(i):
                d_copy(i).wait_recv()
                if swapped(i):
                    @pl.when(heavy)
                    def _():
                        f_copy(i).wait_recv()
                else:
                    f_copy(i).wait_recv()

            at_step(s, near, nb, ready)
            diag_step(s)

        @pl.loop(0, near)
        def _(s):
            def ready(i):
                pass_on(i)
                d_copy(i).wait_recv()
                f_copy(i).wait_recv()

            at_step(s, 0, near, ready)
            for copy in (m_copy, u_copy, v_copy):
                copy(s).wait_recv()
            own_step(s)
            finish(s, False)

        @pl.loop(near, nb)
        def _(j):
            p_copy(j).wait_recv()
            finish(j, True)

        o_copy_out(nb - 2).wait()
        o_copy_out(nb - 1).wait()
        for s in range(nb):
            y_copy(s).wait_send()
            d_copy(s).wait_send()
            f_copy(s).wait_send()
            b1_copy(s).wait_send()
        for s in range(near, nb):
            @pl.when(gives0)
            def _():
                l0_copy(s).wait_send()

            @pl.when(over2(s))
            def _():
                l2_copy(s).wait_send()

            if swapped(s):
                @pl.when(light)
                def _():
                    l3_copy(s).wait_send()

    @pl.when(jnp.logical_not(is_end))
    def _():
        for n in range(AHEAD):
            o_copy(n).start()
        for n in range(near):
            m_copy(n).start()
        for s in range(nb):
            y_copy(s).start()
        for s in range(nb):
            d_copy(s).start()
        acc[...] = jnp.zeros_like(acc)
        part[...] = jnp.zeros_like(part)

        def relay(i):
            @pl.when(has0)
            def _():
                l0_copy(i).wait_recv()
                e0_copy(i).start()

            @pl.when(got2(i))
            def _():
                l2_copy(i).wait_recv()
                e2_copy(i).start()

            if swapped(i):
                @pl.when(light_there)
                def _():
                    l3_copy(i).wait_recv()
                    e3_copy(i).start()

        def relayed(i):
            @pl.when(sib != ze)
            def _():
                e0_copy(i).wait_recv()

            if swapped(i):
                @pl.when(heavy_there)
                def _():
                    e3_copy(i).wait_recv()

            from_sib = jnp.logical_and(3 - c != ze, heavy_there) if swapped(i) else 3 - c != ze

            @pl.when(from_sib)
            def _():
                e2_copy(i).wait_recv()

        def ready(i):
            d_copy(i).wait_recv()
            f_copy(i).wait_recv()

        @pl.loop(0, nb + 4)
        def _(n):
            @pl.when(n < nb)
            def _():
                b1_copy(n).wait_recv()
                w_copy(n).start()

                @pl.when(n + AHEAD < nb)
                def _():
                    o_copy(n + AHEAD).start()

                o_copy(n).wait_recv()
                w_copy(n).wait_recv()

                @pl.when(n < near)
                def _():
                    u_copy(n).start()
                    v_copy(n).start()

                at_step(n, near, nb, relay)

            @pl.when(jnp.logical_and(n > near, n <= nb))
            def _():
                at_step(n - 1, near, nb, relayed)
                end_step(n - 1)

            @pl.when(n == 1)
            def _():
                pass_on(0)

            @pl.when(jnp.logical_and(n >= 2, jnp.logical_and(n != 4, n != 6)))
            def _():
                s = n - 2 - (n > 3).astype(jnp.int32) - (n > 5).astype(jnp.int32)
                at_step(s, 0, nb, ready)
                own_step(s)
                finish(s, False)
                at_step(s + 1, 1, nb, pass_on)

        o_copy_out(nb - 2).wait()
        o_copy_out(nb - 1).wait()
        for s in range(nb):
            y_copy(s).wait_send()
            d_copy(s).wait_send()
            f_copy(s).wait_send()
            o_copy(s).wait_send()
            w_copy(s).wait_send()
        for s in range(near):
            m_copy(s).wait_send()
            u_copy(s).wait_send()
            v_copy(s).wait_send()
        for s in range(near, nb):
            p_copy(s).wait_send()

            @pl.when(has0)
            def _():
                e0_copy(s).wait_send()

            @pl.when(got2(s))
            def _():
                e2_copy(s).wait_send()

            if swapped(s):
                @pl.when(light_there)
                def _():
                    e3_copy(s).wait_send()


def local_trmm(tri, rhs, bs=BLOCK_SIZE, near=NEAR_STEPS):
    size, cols = rhs.shape
    nb = size // bs
    far = nb - near
    any_spec = pl.BlockSpec(memory_space=pl.ANY)
    counts = [nb] * 8 + [far] * 12 + [nb] * 4 + [near] * 6 + [far] * 2
    return pl.pallas_call(
        functools.partial(kernel, bs, nb, near),
        out_shape=[
            jax.ShapeDtypeStruct((size, cols), jnp.bfloat16),
            jax.ShapeDtypeStruct((3, size, size), jnp.bfloat16),
            jax.ShapeDtypeStruct((4, size, size), jnp.bfloat16),
            jax.ShapeDtypeStruct((4, size, cols), jnp.bfloat16),
        ],
        in_specs=[any_spec] * 2,
        out_specs=[any_spec] * 4,
        scratch_shapes=[
            pltpu.VMEM((size, cols), jnp.float32),
            pltpu.VMEM((far * bs, cols), jnp.float32),
            pltpu.VMEM((SLOTS, bs, 4 * bs), jnp.bfloat16),
            pltpu.VMEM((4 * bs, cols), jnp.bfloat16),
            pltpu.VMEM((2, bs, cols), jnp.bfloat16),
            tuple(pltpu.SemaphoreType.DMA((n,)) for n in counts),
            pltpu.SemaphoreType.DMA((SLOTS, 4)),
            pltpu.SemaphoreType.DMA((4,)),
            pltpu.SemaphoreType.DMA((2,)),
        ],
        compiler_params=pltpu.CompilerParams(has_side_effects=True, vmem_limit_bytes=56 * 2**20),
    )(tri, rhs)[0]


def solution(mesh):
    part_spec = P(("batch", "row"), "col")
    return jax.shard_map(local_trmm, mesh=mesh, in_specs=(part_spec, part_spec), out_specs=part_spec, check_vma=False)
```

```python
import functools

import jax
import jax.numpy as jnp
from jax import lax
from jax.experimental import pallas as pl
from jax.experimental.pallas import tpu as pltpu
from jax.sharding import PartitionSpec as P

BLOCK_SIZE = 256
NEAR_STEPS = 6
AHEAD = 1
SLOTS = 5
MESH = pl.DeviceIdType.MESH


def flip(v, t):
    if t == 0:
        return v
    if t == 1:
        return v + 1 - 2 * lax.rem(v, 2)
    if t == 2:
        return lax.rem(v + 2, 4)
    return 3 - v


def xor(a, b):
    return lax.rem(a + b, 2) + 2 * lax.rem(a // 2 + b // 2, 2)


def kernel(bs, nb, near, tri, rhs, out, l_got, l_end, b_got, acc, part, l_tile, b_tile, sems, l_sem, b_sem):
    (ys, yr, ds, dr, fs, fr, b1s, b1r, l0s, l0r, l2s, l2r, e0s, e0r, e2s, e2r, l3s, l3r, e3s, e3r,
     os_, or_, ws, wr, ms, mr, us, ur, vs, vr, ps, pr) = sems
    g, z, c = lax.axis_index("batch"), lax.axis_index("row"), lax.axis_index("col")
    is_end = lax.rem(z, 3) == 0
    ze = flip(z, 1)
    zo = flip(z, 3)
    sib, across = flip(c, 1), flip(c, 2)

    barrier = pltpu.get_barrier_semaphore()
    for peer in ((g, z, sib), (g, z, across), (g, ze, c)):
        pl.semaphore_signal(barrier, inc=1, device_id=peer, device_id_type=MESH)

    @pl.when(jnp.logical_not(is_end))
    def _():
        pl.semaphore_signal(barrier, inc=1, device_id=(g, zo, c), device_id_type=MESH)
        pl.semaphore_wait(barrier, 4)

    @pl.when(is_end)
    def _():
        pl.semaphore_wait(barrier, 3)

    def rows(s):
        return pl.ds(pl.multiple_of(s * bs, bs), bs)

    def panel(ref, s, n=None):
        at = (pl.ds(s * bs, (nb - s) * bs), pl.ds(s * bs, bs))
        return ref.at[at] if n is None else ref.at[(n,) + at]

    def send(src, dst, ss, rs, dev):
        return pltpu.make_async_remote_copy(src_ref=src, dst_ref=dst, send_sem=ss, recv_sem=rs, device_id=dev, device_id_type=MESH)

    def y_copy(s):
        return send(panel(tri, s), panel(l_got, s, 1), ys.at[s], yr.at[s], (g, z, across))

    def d_copy(s):
        return send(panel(tri, s), panel(l_got, s, 0), ds.at[s], dr.at[s], (g, z, sib))

    def f_copy(s):
        return send(panel(l_got, s, 1), panel(l_got, s, 2), fs.at[s], fr.at[s], (g, z, sib))

    def l0_copy(s):
        return send(panel(tri, s), panel(l_end, s, 0), l0s.at[s - near], l0r.at[s - near], (g, ze, c))

    def l2_copy(s):
        return send(panel(l_got, s, 1), panel(l_end, s, 2), l2s.at[s - near], l2r.at[s - near], (g, ze, c))

    def e0_copy(s):
        return send(panel(l_end, s, 0), panel(l_end, s, 1), e0s.at[s - near], e0r.at[s - near], (g, z, sib))

    def e2_copy(s):
        return send(panel(l_end, s, 2), panel(l_end, s, 3), e2s.at[s - near], e2r.at[s - near], (g, z, sib))

    def l3_copy(s):
        return send(panel(l_got, s, 2), panel(l_end, s, 3), l3s.at[s - near], l3r.at[s - near], (g, ze, c))

    def e3_copy(s):
        return send(panel(l_end, s, 3), panel(l_end, s, 2), e3s.at[s - near], e3r.at[s - near], (g, z, sib))

    def b_copy(owner, n, ss, rs, dev):
        return send(rhs.at[rows(n)], b_got.at[owner, rows(n)], ss.at[n], rs.at[n], dev)

    def b_forward(owner, n, ss, rs, dev):
        return send(b_got.at[owner, rows(n)], b_got.at[owner, rows(n)], ss.at[n], rs.at[n], dev)

    def b1_copy(n):
        return b_copy(z, n, b1s, b1r, (g, ze, c))

    def o_copy(n):
        return b_copy(z, n, os_, or_, (g, zo, c))

    def w_copy(n):
        return b_forward(ze, n, ws, wr, (g, zo, c))

    def m_copy(n):
        return b_copy(z, n, ms, mr, (g, ze, c))

    def u_copy(n):
        return b_forward(zo, n, us, ur, (g, ze, c))

    def v_copy(n):
        return b_forward(flip(zo, 1), n, vs, vr, (g, ze, c))

    def p_copy(j):
        at = pl.ds(pl.multiple_of((j - near) * bs, bs), bs)
        return send(part.at[at], part.at[at], ps.at[j - near], pr.at[j - near], (g, ze, c))

    def at_step(s, lo, hi, fn):
        for i in range(lo, hi):
            @pl.when(s == i)
            def _():
                fn(i)

    def pass_on(s):
        y_copy(s).wait_recv()
        f_copy(s).start()

    def load_b(slots):
        for i, owner in slots:
            to = b_tile.at[pl.ds(i * bs, bs)]

            @pl.when(owner == z)
            def _():
                pltpu.make_async_copy(rhs.at[rows(load_b.step)], to, b_sem.at[i]).start()

            @pl.when(owner != z)
            def _():
                pltpu.make_async_copy(b_got.at[owner, rows(load_b.step)], to, b_sem.at[i]).start()

    def tiles(s, start_tile, depth, target, base, after_first=None):
        def start(j):
            start_tile(j, lax.rem(j - s, SLOTS))

        def wait(slot):
            for i in range(depth):
                to = l_tile.at[slot, :, pl.ds(i * bs, bs)]
                pltpu.make_async_copy(tri.at[pl.ds(0, bs), pl.ds(0, bs)], to, l_sem.at[slot, i]).wait()

        for d in range(SLOTS - 1):
            @pl.when(s + d < nb)
            def _():
                start(s + d)
        for i in range(depth):
            pltpu.make_async_copy(rhs.at[rows(0)], b_tile.at[pl.ds(i * bs, bs)], b_sem.at[i]).wait()

        @pl.loop(s, nb)
        def _(j):
            @pl.when(j + SLOTS - 1 < nb)
            def _():
                start(j + SLOTS - 1)

            slot = lax.rem(j - s, SLOTS)
            wait(slot)
            if after_first is not None:
                @pl.when(j == s + 1)
                def _():
                    after_first()

            at = pl.ds(pl.multiple_of((j - base) * bs, bs), bs)
            target[at, :] += jnp.dot(
                l_tile[slot, :, : depth * bs], b_tile[: depth * bs, :], preferred_element_type=jnp.float32
            )

    def l_copy(ref, j, s, slot, i):
        to = l_tile.at[slot, :, pl.ds(i * bs, bs)]
        return pltpu.make_async_copy(ref.at[rows(j), rows(s)], to, l_sem.at[slot, i])

    def own_step(s):
        load_b.step = s
        load_b([(r, flip(c, r)) for r in range(4)])

        def start_tile(j, slot):
            l_copy(tri, j, s, slot, 0).start()
            for r in range(1, 4):
                l_copy(l_got.at[r - 1], j, s, slot, r).start()

        tiles(s, start_tile, 4, acc, 0)

    def diag_step(s):
        load_b.step = s
        load_b([(0, z)])
        r = xor(c, z)

        def start_tile(j, slot):
            @pl.when(r == 0)
            def _():
                l_copy(tri, j, s, slot, 0).start()

            for k in range(1, 4):
                @pl.when(r == k)
                def _():
                    l_copy(l_got.at[k - 1], j, s, slot, 0).start()

        tiles(s, start_tile, 1, acc, 0)

    def end_step(s):
        load_b.step = s
        load_b([(t - 1, flip(ze, t)) for t in range(1, 4)])
        r0 = xor(c, ze)

        def start_tile(j, slot):
            for t in range(1, 4):
                l_copy(l_end.at[flip(r0, t)], j, s, slot, t - 1).start()

        tiles(s, start_tile, 3, part, near, lambda: p_copy(s).start())

        @pl.when(s == nb - 1)
        def _():
            p_copy(s).start()

    def finish(j, extra):
        at = rows(j)
        total = acc[at, :]
        if extra:
            total = total + part[pl.ds(pl.multiple_of((j - near) * bs, bs), bs), :]
        out[at, :] = total.astype(out.dtype)

    gives0, gives2 = c != z, across != z
    has0, has2 = c != ze, across != ze
    light = lax.rem(c + z, 2) == 0
    light_there = lax.rem(c + ze, 2) == 0
    heavy, heavy_there = jnp.logical_not(light), jnp.logical_not(light_there)

    def swapped(s):
        return (s - near) % 2 == 1

    def over2(s):
        return jnp.logical_and(gives2, light) if swapped(s) else gives2

    def got2(s):
        return jnp.logical_and(has2, light_there) if swapped(s) else has2

    @pl.when(is_end)
    def _():
        for s in list(range(near, nb)) + list(range(near)):
            y_copy(s).start()
        for s in range(nb):
            d_copy(s).start()
        order = sorted([(2 * n - 1, n, False) for n in range(nb)] + [(2 * j + 2, j, True) for j in range(near, nb)])
        for _, i, is_l in order:
            if not is_l:
                b1_copy(i).start()
                continue
            pass_on(i)

            @pl.when(gives0)
            def _():
                l0_copy(i).start()

            @pl.when(over2(i))
            def _():
                l2_copy(i).start()

            if swapped(i):
                @pl.when(light)
                def _():
                    f_copy(i).wait_recv()
                    l3_copy(i).start()

        acc[...] = jnp.zeros_like(acc)

        @pl.loop(near, nb)
        def _(s):
            def ready(i):
                d_copy(i).wait_recv()
                if swapped(i):
                    @pl.when(heavy)
                    def _():
                        f_copy(i).wait_recv()
                else:
                    f_copy(i).wait_recv()

            at_step(s, near, nb, ready)
            diag_step(s)

        @pl.loop(0, near)
        def _(s):
            def ready(i):
                pass_on(i)
                d_copy(i).wait_recv()
                f_copy(i).wait_recv()

            at_step(s, 0, near, ready)
            for copy in (m_copy, u_copy, v_copy):
                copy(s).wait_recv()
            own_step(s)
            finish(s, False)

        @pl.loop(near, nb)
        def _(j):
            p_copy(j).wait_recv()
            finish(j, True)

        for s in range(nb):
            y_copy(s).wait_send()
            d_copy(s).wait_send()
            f_copy(s).wait_send()
            b1_copy(s).wait_send()
        for s in range(near, nb):
            @pl.when(gives0)
            def _():
                l0_copy(s).wait_send()

            @pl.when(over2(s))
            def _():
                l2_copy(s).wait_send()

            if swapped(s):
                @pl.when(light)
                def _():
                    l3_copy(s).wait_send()

    @pl.when(jnp.logical_not(is_end))
    def _():
        for n in range(AHEAD):
            o_copy(n).start()
        for n in range(near):
            m_copy(n).start()
        for s in range(nb):
            y_copy(s).start()
        for s in range(nb):
            d_copy(s).start()
        acc[...] = jnp.zeros_like(acc)
        part[...] = jnp.zeros_like(part)

        def relay(i):
            @pl.when(has0)
            def _():
                l0_copy(i).wait_recv()
                e0_copy(i).start()

            @pl.when(got2(i))
            def _():
                l2_copy(i).wait_recv()
                e2_copy(i).start()

            if swapped(i):
                @pl.when(light_there)
                def _():
                    l3_copy(i).wait_recv()
                    e3_copy(i).start()

        def relayed(i):
            @pl.when(sib != ze)
            def _():
                e0_copy(i).wait_recv()

            if swapped(i):
                @pl.when(heavy_there)
                def _():
                    e3_copy(i).wait_recv()

            from_sib = jnp.logical_and(3 - c != ze, heavy_there) if swapped(i) else 3 - c != ze

            @pl.when(from_sib)
            def _():
                e2_copy(i).wait_recv()

        def ready(i):
            d_copy(i).wait_recv()
            f_copy(i).wait_recv()

        b1_copy(0).wait_recv()
        w_copy(0).start()
        o_copy(AHEAD).start()

        @pl.loop(0, nb + 4)
        def _(n):
            @pl.when(n < nb)
            def _():
                @pl.when(n + 1 < nb)
                def _():
                    b1_copy(n + 1).wait_recv()
                    w_copy(n + 1).start()

                @pl.when(n + 1 + AHEAD < nb)
                def _():
                    o_copy(n + 1 + AHEAD).start()

                o_copy(n).wait_recv()
                w_copy(n).wait_recv()

                @pl.when(n < near)
                def _():
                    u_copy(n).start()
                    v_copy(n).start()

                at_step(n, near, nb, relay)

            @pl.when(jnp.logical_and(n > near, n <= nb))
            def _():
                at_step(n - 1, near, nb, relayed)
                end_step(n - 1)

            @pl.when(n == 1)
            def _():
                pass_on(0)

            @pl.when(jnp.logical_and(n >= 2, jnp.logical_and(n != 4, n != 6)))
            def _():
                s = n - 2 - (n > 3).astype(jnp.int32) - (n > 5).astype(jnp.int32)
                at_step(s, 0, nb, ready)
                own_step(s)
                finish(s, False)
                at_step(s + 1, 1, nb, pass_on)

        for s in range(nb):
            y_copy(s).wait_send()
            d_copy(s).wait_send()
            f_copy(s).wait_send()
            o_copy(s).wait_send()
            w_copy(s).wait_send()
        for s in range(near):
            m_copy(s).wait_send()
            u_copy(s).wait_send()
            v_copy(s).wait_send()
        for s in range(near, nb):
            p_copy(s).wait_send()

            @pl.when(has0)
            def _():
                e0_copy(s).wait_send()

            @pl.when(got2(s))
            def _():
                e2_copy(s).wait_send()

            if swapped(s):
                @pl.when(light_there)
                def _():
                    e3_copy(s).wait_send()


def local_trmm(tri, rhs, bs=BLOCK_SIZE, near=NEAR_STEPS):
    size, cols = rhs.shape
    nb = size // bs
    far = nb - near
    any_spec = pl.BlockSpec(memory_space=pl.ANY)
    counts = [nb] * 8 + [far] * 12 + [nb] * 4 + [near] * 6 + [far] * 2
    return pl.pallas_call(
        functools.partial(kernel, bs, nb, near),
        out_shape=[
            pltpu.VMEM((size, cols), jnp.bfloat16),
            jax.ShapeDtypeStruct((3, size, size), jnp.bfloat16),
            jax.ShapeDtypeStruct((4, size, size), jnp.bfloat16),
            jax.ShapeDtypeStruct((4, size, cols), jnp.bfloat16),
        ],
        in_specs=[any_spec] * 2,
        out_specs=[pl.BlockSpec(memory_space=pltpu.VMEM)] + [any_spec] * 3,
        scratch_shapes=[
            pltpu.VMEM((size, cols), jnp.float32),
            pltpu.VMEM((far * bs, cols), jnp.float32),
            pltpu.VMEM((SLOTS, bs, 4 * bs), jnp.bfloat16),
            pltpu.VMEM((4 * bs, cols), jnp.bfloat16),
            tuple(pltpu.SemaphoreType.DMA((n,)) for n in counts),
            pltpu.SemaphoreType.DMA((SLOTS, 4)),
            pltpu.SemaphoreType.DMA((4,)),
        ],
        compiler_params=pltpu.CompilerParams(has_side_effects=True, collective_id=0, vmem_limit_bytes=48 * 2**20),
    )(tri, rhs)[0]


def solution(mesh):
    part_spec = P(("batch", "row"), "col")
    return jax.shard_map(local_trmm, mesh=mesh, in_specs=(part_spec, part_spec), out_specs=part_spec, check_vma=False)
```

```python
import functools

import jax
import jax.numpy as jnp
from jax import lax
from jax.experimental import pallas as pl
from jax.experimental.pallas import tpu as pltpu
from jax.sharding import PartitionSpec as P

BLOCK_SIZE = 256
NEAR_STEPS = 5
VIA_Y = 3
EARLY = 3
AHEAD = 1
SLOTS = 5
MESH = pl.DeviceIdType.MESH


def flip(v, t):
    if t == 0:
        return v
    if t == 1:
        return v + 1 - 2 * lax.rem(v, 2)
    if t == 2:
        return lax.rem(v + 2, 4)
    return 3 - v


def xor(a, b):
    return lax.rem(a + b, 2) + 2 * lax.rem(a // 2 + b // 2, 2)


def kernel(bs, nb, near, tri, rhs, out, l_got, l_end, b_got, acc, part, l_tile, b_tile, sems, l_sem, b_sem):
    (ys, yr, ds, dr, fs, fr, b1s, b1r, l0s, l0r, l2s, l2r, e0s, e0r, e2s, e2r, l3s, l3r, e3s, e3r, y2s, y2r,
     os_, or_, ws, wr, ms, mr, us, ur, vs, vr, ps, pr) = sems
    g, z, c = lax.axis_index("batch"), lax.axis_index("row"), lax.axis_index("col")
    is_end = lax.rem(z, 3) == 0
    ze = flip(z, 1)
    zo = flip(z, 3)
    sib, across = flip(c, 1), flip(c, 2)

    barrier = pltpu.get_barrier_semaphore()
    for peer in ((g, z, sib), (g, z, across), (g, ze, c)):
        pl.semaphore_signal(barrier, inc=1, device_id=peer, device_id_type=MESH)

    @pl.when(jnp.logical_not(is_end))
    def _():
        pl.semaphore_signal(barrier, inc=1, device_id=(g, zo, c), device_id_type=MESH)
        pl.semaphore_wait(barrier, 4)

    @pl.when(is_end)
    def _():
        pl.semaphore_wait(barrier, 3)

    def rows(s):
        return pl.ds(pl.multiple_of(s * bs, bs), bs)

    def panel(ref, s, n=None):
        at = (pl.ds(s * bs, (nb - s) * bs), pl.ds(s * bs, bs))
        return ref.at[at] if n is None else ref.at[(n,) + at]

    def send(src, dst, ss, rs, dev):
        return pltpu.make_async_remote_copy(src_ref=src, dst_ref=dst, send_sem=ss, recv_sem=rs, device_id=dev, device_id_type=MESH)

    def y_copy(s):
        return send(panel(tri, s), panel(l_got, s, 1), ys.at[s], yr.at[s], (g, z, across))

    def d_copy(s):
        return send(panel(tri, s), panel(l_got, s, 0), ds.at[s], dr.at[s], (g, z, sib))

    def f_copy(s):
        return send(panel(l_got, s, 1), panel(l_got, s, 2), fs.at[s], fr.at[s], (g, z, sib))

    def l0_copy(s):
        return send(panel(tri, s), panel(l_end, s, 0), l0s.at[s - near], l0r.at[s - near], (g, ze, c))

    def l2_copy(s):
        return send(panel(l_got, s, 1), panel(l_end, s, 2), l2s.at[s - near], l2r.at[s - near], (g, ze, c))

    def e0_copy(s):
        return send(panel(l_end, s, 0), panel(l_end, s, 1), e0s.at[s - near], e0r.at[s - near], (g, z, sib))

    def e2_copy(s):
        return send(panel(l_end, s, 2), panel(l_end, s, 3), e2s.at[s - near], e2r.at[s - near], (g, z, sib))

    def l3_copy(s):
        return send(panel(l_got, s, 2), panel(l_end, s, 3), l3s.at[s - near], l3r.at[s - near], (g, ze, c))

    def e3_copy(s):
        return send(panel(l_end, s, 3), panel(l_end, s, 2), e3s.at[s - near], e3r.at[s - near], (g, z, sib))

    def y2_copy(s):
        return send(panel(l_end, s, 0), panel(l_end, s, 2), y2s.at[s - near], y2r.at[s - near], (g, z, across))

    def b_copy(owner, n, ss, rs, dev):
        return send(rhs.at[rows(n)], b_got.at[owner, rows(n)], ss.at[n], rs.at[n], dev)

    def b_forward(owner, n, ss, rs, dev):
        return send(b_got.at[owner, rows(n)], b_got.at[owner, rows(n)], ss.at[n], rs.at[n], dev)

    def b1_copy(n):
        return b_copy(z, n, b1s, b1r, (g, ze, c))

    def o_copy(n):
        return b_copy(z, n, os_, or_, (g, zo, c))

    def w_copy(n):
        return b_forward(ze, n, ws, wr, (g, zo, c))

    def m_copy(n):
        return b_copy(z, n, ms, mr, (g, ze, c))

    def u_copy(n):
        return b_forward(zo, n, us, ur, (g, ze, c))

    def v_copy(n):
        return b_forward(flip(zo, 1), n, vs, vr, (g, ze, c))

    def p_copy(j):
        at = pl.ds(pl.multiple_of((j - near) * bs, bs), bs)
        return send(part.at[at], part.at[at], ps.at[j - near], pr.at[j - near], (g, ze, c))

    def at_step(s, lo, hi, fn):
        for i in range(lo, hi):
            @pl.when(s == i)
            def _():
                fn(i)

    def pass_on(s):
        y_copy(s).wait_recv()
        f_copy(s).start()

    def load_b(slots):
        for i, owner in slots:
            to = b_tile.at[pl.ds(i * bs, bs)]

            @pl.when(owner == z)
            def _():
                pltpu.make_async_copy(rhs.at[rows(load_b.step)], to, b_sem.at[i]).start()

            @pl.when(owner != z)
            def _():
                pltpu.make_async_copy(b_got.at[owner, rows(load_b.step)], to, b_sem.at[i]).start()

    def tiles(s, start_tile, depth, target, base, after_first=None):
        def start(j):
            start_tile(j, lax.rem(j - s, SLOTS))

        def wait(slot):
            for i in range(depth):
                to = l_tile.at[slot, :, pl.ds(i * bs, bs)]
                pltpu.make_async_copy(tri.at[pl.ds(0, bs), pl.ds(0, bs)], to, l_sem.at[slot, i]).wait()

        for d in range(SLOTS - 1):
            @pl.when(s + d < nb)
            def _():
                start(s + d)
        for i in range(depth):
            pltpu.make_async_copy(rhs.at[rows(0)], b_tile.at[pl.ds(i * bs, bs)], b_sem.at[i]).wait()

        @pl.loop(s, nb)
        def _(j):
            @pl.when(j + SLOTS - 1 < nb)
            def _():
                start(j + SLOTS - 1)

            slot = lax.rem(j - s, SLOTS)
            wait(slot)
            if after_first is not None:
                @pl.when(j == s + 1)
                def _():
                    after_first()

            at = pl.ds(pl.multiple_of((j - base) * bs, bs), bs)
            target[at, :] += jnp.dot(
                l_tile[slot, :, : depth * bs], b_tile[: depth * bs, :], preferred_element_type=jnp.float32
            )

    def l_copy(ref, j, s, slot, i):
        to = l_tile.at[slot, :, pl.ds(i * bs, bs)]
        return pltpu.make_async_copy(ref.at[rows(j), rows(s)], to, l_sem.at[slot, i])

    def own_step(s):
        load_b.step = s
        load_b([(r, flip(c, r)) for r in range(4)])

        def start_tile(j, slot):
            l_copy(tri, j, s, slot, 0).start()
            for r in range(1, 4):
                l_copy(l_got.at[r - 1], j, s, slot, r).start()

        tiles(s, start_tile, 4, acc, 0)

    def diag_step(s):
        load_b.step = s
        load_b([(0, z)])
        r = xor(c, z)

        def start_tile(j, slot):
            @pl.when(r == 0)
            def _():
                l_copy(tri, j, s, slot, 0).start()

            for k in range(1, 4):
                @pl.when(r == k)
                def _():
                    l_copy(l_got.at[k - 1], j, s, slot, 0).start()

        tiles(s, start_tile, 1, acc, 0)

    def end_step(s):
        load_b.step = s
        load_b([(t - 1, flip(ze, t)) for t in range(1, 4)])
        r0 = xor(c, ze)

        def start_tile(j, slot):
            for t in range(1, 4):
                l_copy(l_end.at[flip(r0, t)], j, s, slot, t - 1).start()

        tiles(s, start_tile, 3, part, near, lambda: p_copy(s).start())

        @pl.when(s == nb - 1)
        def _():
            p_copy(s).start()

    def finish(j, extra):
        at = rows(j)
        total = acc[at, :]
        if extra:
            total = total + part[pl.ds(pl.multiple_of((j - near) * bs, bs), bs), :]
        out[at, :] = total.astype(out.dtype)

    gives0, gives2 = c != z, across != z
    has0, has2 = c != ze, across != ze
    light = lax.rem(c + z, 2) == 0
    light_there = lax.rem(c + ze, 2) == 0
    heavy, heavy_there = jnp.logical_not(light), jnp.logical_not(light_there)

    def via_y(s):
        return s < near + VIA_Y

    def swapped(s):
        return not via_y(s) and (s - near) % 2 == 1

    def over2(s):
        return jnp.logical_and(gives2, light) if swapped(s) else gives2

    def got2(s):
        return jnp.logical_and(has2, light_there) if swapped(s) else has2

    @pl.when(is_end)
    def _():
        for s in list(range(near, nb)) + list(range(near)):
            y_copy(s).start()
        for s in range(nb):
            d_copy(s).start()
        order = sorted([(2 * n - 1, n, False) for n in range(nb)] + [(2 * j + (0 if via_y(j) else 2), j, True) for j in range(near, nb)])
        for _, i, is_l in order:
            if not is_l:
                b1_copy(i).start()
                continue
            pass_on(i)

            @pl.when(gives0)
            def _():
                l0_copy(i).start()

            if via_y(i):
                continue

            @pl.when(over2(i))
            def _():
                l2_copy(i).start()

            if swapped(i):
                @pl.when(light)
                def _():
                    f_copy(i).wait_recv()
                    l3_copy(i).start()

        acc[...] = jnp.zeros_like(acc)

        @pl.loop(near, nb)
        def _(s):
            def ready(i):
                d_copy(i).wait_recv()
                if swapped(i):
                    @pl.when(heavy)
                    def _():
                        f_copy(i).wait_recv()
                else:
                    f_copy(i).wait_recv()

            at_step(s, near, nb, ready)
            diag_step(s)

        @pl.loop(0, near)
        def _(s):
            def ready(i):
                pass_on(i)
                d_copy(i).wait_recv()
                f_copy(i).wait_recv()

            at_step(s, 0, near, ready)
            for copy in (m_copy, u_copy, v_copy):
                copy(s).wait_recv()
            own_step(s)
            finish(s, False)

        @pl.loop(near, nb)
        def _(j):
            p_copy(j).wait_recv()
            finish(j, True)

        for s in range(nb):
            y_copy(s).wait_send()
            d_copy(s).wait_send()
            f_copy(s).wait_send()
            b1_copy(s).wait_send()
        for s in range(near, nb):
            @pl.when(gives0)
            def _():
                l0_copy(s).wait_send()

            if via_y(s):
                continue

            @pl.when(over2(s))
            def _():
                l2_copy(s).wait_send()

            if swapped(s):
                @pl.when(light)
                def _():
                    l3_copy(s).wait_send()

    @pl.when(jnp.logical_not(is_end))
    def _():
        for n in range(AHEAD):
            o_copy(n).start()
        for n in range(near):
            m_copy(n).start()
        for s in range(EARLY):
            y_copy(s).start()
        for s in range(nb):
            d_copy(s).start()
        acc[...] = jnp.zeros_like(acc)
        part[...] = jnp.zeros_like(part)

        def relay(i):
            @pl.when(has0)
            def _():
                l0_copy(i).wait_recv()
                if via_y(i):
                    y2_copy(i).start()
                e0_copy(i).start()

            if i == near + VIA_Y - 1:
                for s in range(EARLY, nb):
                    y_copy(s).start()
            if via_y(i):
                return

            @pl.when(got2(i))
            def _():
                l2_copy(i).wait_recv()
                e2_copy(i).start()

            if swapped(i):
                @pl.when(light_there)
                def _():
                    l3_copy(i).wait_recv()
                    e3_copy(i).start()

        def crossed(i):
            @pl.when(has2)
            def _():
                y2_copy(i).wait_recv()
                e2_copy(i).start()

        def relayed(i):
            @pl.when(sib != ze)
            def _():
                e0_copy(i).wait_recv()

            if swapped(i):
                @pl.when(heavy_there)
                def _():
                    e3_copy(i).wait_recv()

            from_sib = jnp.logical_and(3 - c != ze, heavy_there) if swapped(i) else 3 - c != ze

            @pl.when(from_sib)
            def _():
                e2_copy(i).wait_recv()

        def ready(i):
            d_copy(i).wait_recv()
            f_copy(i).wait_recv()

        b1_copy(0).wait_recv()
        w_copy(0).start()
        o_copy(AHEAD).start()

        @pl.loop(0, nb + 5)
        def _(n):
            @pl.when(n < nb)
            def _():
                @pl.when(n + 1 < nb)
                def _():
                    b1_copy(n + 1).wait_recv()
                    w_copy(n + 1).start()

                @pl.when(n + 1 + AHEAD < nb)
                def _():
                    o_copy(n + 1 + AHEAD).start()

                o_copy(n).wait_recv()
                w_copy(n).wait_recv()

                @pl.when(n < near)
                def _():
                    u_copy(n).start()
                    v_copy(n).start()

                at_step(n + 1, near, near + VIA_Y, relay)
                at_step(n, near, near + VIA_Y, crossed)
                at_step(n, near + VIA_Y, nb, relay)

            @pl.when(jnp.logical_and(n >= near, n < nb))
            def _():
                at_step(n, near, nb, relayed)
                end_step(n)

            @pl.when(jnp.logical_and(n >= 2, jnp.logical_and(n != 4, jnp.logical_or(n < 6, n > 7))))
            def _():
                s = n - 2 - (n > 3).astype(jnp.int32) - 2 * (n > 5).astype(jnp.int32)
                at_step(s, 0, nb, ready)
                own_step(s)
                finish(s, False)

            at_step(n - 1, 0, 2, pass_on)
            at_step(n - 2, 2, 3, pass_on)
            at_step(n - 4, 3, nb, pass_on)

        for s in range(nb):
            y_copy(s).wait_send()
            d_copy(s).wait_send()
            f_copy(s).wait_send()
            o_copy(s).wait_send()
            w_copy(s).wait_send()
        for s in range(near):
            m_copy(s).wait_send()
            u_copy(s).wait_send()
            v_copy(s).wait_send()
        for s in range(near, nb):
            p_copy(s).wait_send()

            @pl.when(has0)
            def _():
                e0_copy(s).wait_send()
                if via_y(s):
                    y2_copy(s).wait_send()

            @pl.when(has2 if via_y(s) else got2(s))
            def _():
                e2_copy(s).wait_send()

            if swapped(s):
                @pl.when(light_there)
                def _():
                    e3_copy(s).wait_send()


def local_trmm(tri, rhs, bs=BLOCK_SIZE, near=NEAR_STEPS):
    size, cols = rhs.shape
    nb = size // bs
    far = nb - near
    any_spec = pl.BlockSpec(memory_space=pl.ANY)
    counts = [nb] * 8 + [far] * 14 + [nb] * 4 + [near] * 6 + [far] * 2
    return pl.pallas_call(
        functools.partial(kernel, bs, nb, near),
        out_shape=[
            pltpu.VMEM((size, cols), jnp.bfloat16),
            jax.ShapeDtypeStruct((3, size, size), jnp.bfloat16),
            jax.ShapeDtypeStruct((4, size, size), jnp.bfloat16),
            jax.ShapeDtypeStruct((4, size, cols), jnp.bfloat16),
        ],
        in_specs=[any_spec] * 2,
        out_specs=[pl.BlockSpec(memory_space=pltpu.VMEM)] + [any_spec] * 3,
        scratch_shapes=[
            pltpu.VMEM((size, cols), jnp.float32),
            pltpu.VMEM((far * bs, cols), jnp.float32),
            pltpu.VMEM((SLOTS, bs, 4 * bs), jnp.bfloat16),
            pltpu.VMEM((4 * bs, cols), jnp.bfloat16),
            tuple(pltpu.SemaphoreType.DMA((n,)) for n in counts),
            pltpu.SemaphoreType.DMA((SLOTS, 4)),
            pltpu.SemaphoreType.DMA((4,)),
        ],
        compiler_params=pltpu.CompilerParams(has_side_effects=True, collective_id=0, vmem_limit_bytes=48 * 2**20),
    )(tri, rhs)[0]


def solution(mesh):
    part_spec = P(("batch", "row"), "col")
    return jax.shard_map(local_trmm, mesh=mesh, in_specs=(part_spec, part_spec), out_specs=part_spec, check_vma=False)
```
